32 devices in a mesh: row: 4 (over z), col: 8 (over y, x, core).
Axes of the slice: x: 2, y: 2, z: 4, core: 2. Of those that a mesh axis runs over, the one named last changes fastest.
Arguments:
- coupling: bfloat16 [32768, 32768], P(('row', 'col')), may hold values from -0.0078125 to 0.0078125
- right_side: float32 [32768, 128], P(('row', 'col')), may hold values from -18 to 18
- precond: float32 [128, 256, 256], P(('row', 'col')), may hold values from -0.09375 to 0.09375
Outputs:
- solution: float32 [32768, 128], P(('row', 'col'))
- norms: float32 [4, 128], replicated
The draws below stay inside these ranges and needn't reach their ends.
All inputs are finite; a program needn't handle non-finite values.
Results may differ from the reference program's by a relative error of at most 0.00082.
Values may be sent and summed in bfloat16 or wider, within the bound.
A program may use at most 128 MiB of HBM per device.

```python
import jax
import jax.numpy as jnp
from jax import lax

N = 32768
NRHS = 128
B = 256
ITERS = 4
NBLK = 128


def draw_right_side(key, part):
    positions = jnp.arange(N, dtype=jnp.float32) / N
    base = jnp.clip(jax.random.normal(key, (N, NRHS), jnp.float32), -6.0, 6.0)
    factor = jnp.exp(jnp.log(3.0) * positions)[:, None]
    return base * factor


def block_levels(rng, extent, pieces, smallest, largest):
    factor_of = 1.0
    for axis_at, blocks in pieces:
        draws = jax.random.uniform(jax.random.fold_in(jax.random.fold_in(rng, 6), axis_at), (blocks,), jnp.float32, smallest / len(pieces), largest / len(pieces))
        factor_of = factor_of * jnp.repeat(jnp.exp(draws), extent[axis_at] // blocks).reshape((-1,) + (1,) * (len(extent) - 1 - axis_at))
    return factor_of


def bell_draw(stream_key, dims, width, reach, cuts=(), held_as=jnp.bfloat16):
    level = block_levels(stream_key, dims, cuts, -0.22, 0.18) if cuts else 1.0
    values = jax.random.normal(stream_key, dims, jnp.float32) * width * level
    return jnp.minimum(jnp.maximum(values, -reach), reach).astype(held_as)


def setup_inputs(seed: int = 0) -> dict:
    seeds = jax.random.split(jax.random.key(seed), 4)
    return {
        "coupling": bell_draw(seeds[0], (N, N), (16 * N) ** -0.5, 0.0078125, ((0, 32),)),
        "right_side": draw_right_side(jax.random.fold_in(seeds[3], 71), 0),
        "precond": bell_draw(seeds[2], (NBLK, B, B), (16 * B) ** -0.5, 0.09375, ((0, 32),), jnp.float32),
    }


def precondition(resid, precond):
    blocks = resid.reshape(precond.shape[0], precond.shape[1], resid.shape[1])
    applied = jnp.einsum('kij,kjn->kin', precond, blocks, precision=lax.Precision.HIGHEST)
    return resid + applied.reshape(resid.shape)

def reference(coupling, right_side, precond):
    solution = jnp.zeros(right_side.shape, jnp.float32)
    collected = []
    for step in range(ITERS):
        if step == 0:
            resid = right_side
        else:
            product = jnp.dot(coupling, solution.astype(jnp.bfloat16), preferred_element_type=jnp.float32)
            resid = right_side - solution - product
        collected.append(jnp.sqrt(lax.optimization_barrier(jnp.sum(resid * resid, axis=0)) / N))
        solution = solution + precondition(resid, precond)
    return (solution, jnp.stack(collected))
```

```python
import functools

import jax
import jax.numpy as jnp
from jax import lax
from jax.experimental import pallas as pl
from jax.experimental.pallas import tpu as pltpu
from jax.sharding import PartitionSpec as P

ITERS = 4
CORES = 2
INNER = 2


def precondition(resid, precond):
    blocks = resid.reshape(precond.shape[0], precond.shape[1], resid.shape[1])
    applied = jnp.einsum("kij,kjn->kin", precond, blocks, precision=lax.Precision.HIGHEST)
    return resid + applied.reshape(resid.shape)


def plan(rows_axis, cols_axis):
    outer = cols_axis // (CORES * INNER)
    plane = [("z", k, 0, 0) for k in range(1, rows_axis)]
    for k in range(rows_axis):
        plane += [("a", k, i, 0) for i in range(1, outer)] + [("b", k, 0, j) for j in range(1, INNER)]
        plane += [(d, k, i, j) for d in "pq" for i in range(1, outer) for j in range(1, INNER)]
    every = plane + [("own", 0, 0, 0)]
    return every + [("core",) + name for name in every]


def gather_kernel(rows_axis, cols_axis, x_ref, out_ref, send_sem, recv_sem):
    outer = cols_axis // (CORES * INNER)
    r, c = lax.axis_index("row"), lax.axis_index("col")
    core, chip = lax.rem(c, CORES), lax.div(c, CORES)
    b, a = lax.rem(chip, INNER), lax.div(chip, INNER)
    rows = x_ref.shape[0]
    half = rows // 2
    number = {name: at for at, name in enumerate(plan(rows_axis, cols_axis))}

    def back(v, k, size):
        return lax.rem(v + size - k, size)

    def ahead(v, k, size):
        return lax.rem(v + k, size)

    def device(r, a, b, core):
        return (r, (a * INNER + b) * CORES + core)

    def shard(k, i, j, part=None, core=core):
        index = back(r, k, rows_axis) * cols_axis + (back(a, i, outer) * INNER + back(b, j, INNER)) * CORES + core
        start, size = index * rows, rows
        if part is not None:
            start, size = start + part * half, half
        return out_ref.at[pl.ds(pl.multiple_of(start, size), size), :]

    peers = [device(ahead(r, k, rows_axis), a, b, core) for k in range(1, rows_axis)]
    over_a = [device(r, ahead(a, i, outer), b, core) for i in range(1, outer)]
    over_b = [device(r, a, ahead(b, j, INNER), core) for j in range(1, INNER)]
    partner = device(r, a, b, 1 - core)

    barrier = pltpu.get_barrier_semaphore()
    everyone = peers + over_a + over_b + [partner]
    for peer in everyone:
        pl.semaphore_signal(barrier, inc=1, device_id=peer, device_id_type=pl.DeviceIdType.MESH)
    pl.semaphore_wait(barrier, len(everyone))

    sent = []

    def copy(src, dst, name, to):
        at = number[name]
        return pltpu.make_async_remote_copy(
            src_ref=src,
            dst_ref=dst,
            send_sem=send_sem.at[at],
            recv_sem=recv_sem.at[at],
            device_id=to,
            device_id_type=pl.DeviceIdType.MESH,
        )

    def send(src, dst, name, to):
        moved = copy(src, dst, name, to)
        moved.start()
        sent.append(moved)

    def arrive(ref, name):
        copy(ref, ref, name, partner).wait_recv()

    def spread(k, src, dst):
        for i in range(1, outer):
            send(src, dst, ("a", k, i, 0), over_a[i - 1])
        for j in range(1, INNER):
            send(src, dst, ("b", k, 0, j), over_b[j - 1])

    mine = shard(0, 0, 0)
    spread(0, x_ref, mine)
    for k in range(1, rows_axis):
        send(x_ref, mine, ("z", k, 0, 0), peers[k - 1])
    send(x_ref, mine, ("core", "own", 0, 0, 0), partner)
    index = r * cols_axis + c
    out_ref[pl.ds(pl.multiple_of(index * rows, rows), rows), :] = x_ref[...]

    for k in range(1, rows_axis):
        ref = shard(k, 0, 0)
        arrive(ref, ("z", k, 0, 0))
        spread(k, ref, ref)
        send(ref, ref, ("core", "z", k, 0, 0), partner)
    for k in range(rows_axis):
        for i in range(1, outer):
            ref = shard(k, i, 0)
            arrive(ref, ("a", k, i, 0))
            for j in range(1, INNER):
                send(shard(k, i, 0, 0), shard(k, i, 0, 0), ("p", k, i, j), over_b[j - 1])
            send(ref, ref, ("core", "a", k, i, 0), partner)
        for j in range(1, INNER):
            ref = shard(k, 0, j)
            arrive(ref, ("b", k, 0, j))
            for i in range(1, outer):
                send(shard(k, 0, j, 1), shard(k, 0, j, 1), ("q", k, i, j), over_a[i - 1])
            send(ref, ref, ("core", "b", k, 0, j), partner)
    for k in range(rows_axis):
        for i in range(1, outer):
            for j in range(1, INNER):
                for part, kind in ((0, "p"), (1, "q")):
                    ref = shard(k, i, j, part)
                    arrive(ref, (kind, k, i, j))
                    send(ref, ref, ("core", kind, k, i, j), partner)

    other = 1 - core
    for name in number:
        if name[0] == "core":
            kind, k, i, j = name[1:]
            part = {"p": 0, "q": 1}.get(kind)
            arrive(shard(k, i, j, part, other), name)
    for moved in sent:
        moved.wait_send()


def gather(x, rows_axis, cols_axis, number):
    copies = len(plan(rows_axis, cols_axis))
    total = rows_axis * cols_axis * x.shape[0]
    return pl.pallas_call(
        functools.partial(gather_kernel, rows_axis, cols_axis),
        out_shape=jax.ShapeDtypeStruct((total, x.shape[1]), x.dtype),
        in_specs=[pl.BlockSpec(memory_space=pltpu.VMEM)],
        out_specs=pl.BlockSpec(memory_space=pltpu.VMEM),
        scratch_shapes=[pltpu.SemaphoreType.DMA((copies,)), pltpu.SemaphoreType.DMA((copies,))],
        compiler_params=pltpu.CompilerParams(collective_id=number, has_side_effects=True),
    )(x)


def local(rows_axis, cols_axis, coupling, right_side, precond):
    total = coupling.shape[1]
    collected = []
    solution = jnp.zeros(right_side.shape, jnp.float32)
    for step in range(ITERS):
        if step == 0:
            resid = right_side
        else:
            everyone = gather(solution.astype(jnp.bfloat16), rows_axis, cols_axis, 0)
            product = jnp.dot(coupling, everyone, preferred_element_type=jnp.float32)
            resid = right_side - solution - product
        collected.append(jnp.sum(resid * resid, axis=0))
        solution = solution + precondition(resid, precond)
    squares = jnp.pad(jnp.stack(collected), ((0, 16 - ITERS), (0, 0)))
    squares = gather(squares, rows_axis, cols_axis, 1).reshape(-1, 16, squares.shape[1])
    norms = jnp.sqrt(jnp.sum(squares[:, :ITERS], axis=0) / total)
    return (solution, norms)


def solution(mesh):
    in_specs = (P(("row", "col"), None), P(("row", "col"), None), P(("row", "col"), None, None))
    out_specs = (P(("row", "col"), None), P())
    body = functools.partial(local, mesh.shape["row"], mesh.shape["col"])
    return jax.shard_map(body, mesh=mesh, in_specs=in_specs, out_specs=out_specs, check_vma=False)
```

```python
import functools

import jax
import jax.numpy as jnp
from jax import lax
from jax.experimental import pallas as pl
from jax.experimental.pallas import tpu as pltpu
from jax.sharding import PartitionSpec as P

ITERS = 4
CORES = 2
INNER = 2


def precondition(resid, precond):
    blocks = resid.reshape(precond.shape[0], precond.shape[1], resid.shape[1])
    applied = jnp.einsum("kij,kjn->kin", precond, blocks, precision=lax.Precision.HIGHEST)
    return resid + applied.reshape(resid.shape)


def plan(rows_axis, cols_axis):
    outer = cols_axis // (CORES * INNER)
    plane = [("z", k, 0, 0) for k in range(1, rows_axis)]
    for k in range(rows_axis):
        plane += [("a", k, i, 0) for i in range(1, outer)] + [("b", k, 0, j) for j in range(1, INNER)]
        plane += [(d, k, i, j) for d in "pq" for i in range(1, outer) for j in range(1, INNER)]
    every = plane + [("own", 0, 0, 0)]
    return every + [("core",) + name for name in every]


def gather_kernel(rows_axis, cols_axis, x_ref, out_ref, send_sem, recv_sem):
    outer = cols_axis // (CORES * INNER)
    r, c = lax.axis_index("row"), lax.axis_index("col")
    core, chip = lax.rem(c, CORES), lax.div(c, CORES)
    b, a = lax.rem(chip, INNER), lax.div(chip, INNER)
    rows = x_ref.shape[0]
    half = rows // 2
    number = {name: at for at, name in enumerate(plan(rows_axis, cols_axis))}

    def back(v, k, size):
        return lax.rem(v + size - k, size)

    def ahead(v, k, size):
        return lax.rem(v + k, size)

    def device(r, a, b, core):
        return (r, (a * INNER + b) * CORES + core)

    def shard(k, i, j, part=None, core=core):
        index = back(r, k, rows_axis) * cols_axis + (back(a, i, outer) * INNER + back(b, j, INNER)) * CORES + core
        start, size = index * rows, rows
        if part is not None:
            start, size = start + part * half, half
        return out_ref.at[pl.ds(pl.multiple_of(start, size), size), :]

    peers = [device(ahead(r, k, rows_axis), a, b, core) for k in range(1, rows_axis)]
    over_a = [device(r, ahead(a, i, outer), b, core) for i in range(1, outer)]
    over_b = [device(r, a, ahead(b, j, INNER), core) for j in range(1, INNER)]
    partner = device(r, a, b, 1 - core)

    barrier = pltpu.get_barrier_semaphore()
    everyone = peers + over_a + over_b + [partner]
    for peer in everyone:
        pl.semaphore_signal(barrier, inc=1, device_id=peer, device_id_type=pl.DeviceIdType.MESH)
    pl.semaphore_wait(barrier, len(everyone))

    sent = []

    def copy(src, dst, name, to):
        at = number[name]
        return pltpu.make_async_remote_copy(
            src_ref=src,
            dst_ref=dst,
            send_sem=send_sem.at[at],
            recv_sem=recv_sem.at[at],
            device_id=to,
            device_id_type=pl.DeviceIdType.MESH,
        )

    def send(src, dst, name, to):
        moved = copy(src, dst, name, to)
        moved.start()
        sent.append(moved)

    def arrive(ref, name):
        copy(ref, ref, name, partner).wait_recv()

    def spread(k, src, dst):
        for i in range(1, outer):
            send(src, dst, ("a", k, i, 0), over_a[i - 1])
        for j in range(1, INNER):
            send(src, dst, ("b", k, 0, j), over_b[j - 1])

    mine = shard(0, 0, 0)
    spread(0, x_ref, mine)
    for k in range(1, rows_axis):
        send(x_ref, mine, ("z", k, 0, 0), peers[k - 1])
    send(x_ref, mine, ("core", "own", 0, 0, 0), partner)
    index = r * cols_axis + c
    out_ref[pl.ds(pl.multiple_of(index * rows, rows), rows), :] = x_ref[...]

    def cross(k):
        for i in range(1, outer):
            ref = shard(k, i, 0)
            arrive(ref, ("a", k, i, 0))
            for j in range(1, INNER):
                send(shard(k, i, 0, 0), shard(k, i, 0, 0), ("p", k, i, j), over_b[j - 1])
            send(ref, ref, ("core", "a", k, i, 0), partner)
        for j in range(1, INNER):
            ref = shard(k, 0, j)
            arrive(ref, ("b", k, 0, j))
            for i in range(1, outer):
                send(shard(k, 0, j, 1), shard(k, 0, j, 1), ("q", k, i, j), over_a[i - 1])
            send(ref, ref, ("core", "b", k, 0, j), partner)

    for k in range(1, rows_axis):
        ref = shard(k, 0, 0)
        arrive(ref, ("z", k, 0, 0))
        spread(k, ref, ref)
        send(ref, ref, ("core", "z", k, 0, 0), partner)
        cross(k - 1)
    cross(rows_axis - 1)
    for k in range(rows_axis):
        for i in range(1, outer):
            for j in range(1, INNER):
                for part, kind in ((0, "p"), (1, "q")):
                    ref = shard(k, i, j, part)
                    arrive(ref, (kind, k, i, j))
                    send(ref, ref, ("core", kind, k, i, j), partner)

    other = 1 - core
    for name in number:
        if name[0] == "core":
            kind, k, i, j = name[1:]
            part = {"p": 0, "q": 1}.get(kind)
            arrive(shard(k, i, j, part, other), name)
    for moved in sent:
        moved.wait_send()


def gather(x, rows_axis, cols_axis, number):
    copies = len(plan(rows_axis, cols_axis))
    total = rows_axis * cols_axis * x.shape[0]
    return pl.pallas_call(
        functools.partial(gather_kernel, rows_axis, cols_axis),
        out_shape=jax.ShapeDtypeStruct((total, x.shape[1]), x.dtype),
        in_specs=[pl.BlockSpec(memory_space=pltpu.VMEM)],
        out_specs=pl.BlockSpec(memory_space=pltpu.VMEM),
        scratch_shapes=[pltpu.SemaphoreType.DMA((copies,)), pltpu.SemaphoreType.DMA((copies,))],
        compiler_params=pltpu.CompilerParams(collective_id=number, has_side_effects=True),
    )(x)


def local(rows_axis, cols_axis, coupling, right_side, precond):
    total = coupling.shape[1]
    collected = []
    solution = jnp.zeros(right_side.shape, jnp.float32)
    for step in range(ITERS):
        if step == 0:
            resid = right_side
        else:
            everyone = gather(solution.astype(jnp.bfloat16), rows_axis, cols_axis, 0)
            product = jnp.dot(coupling, everyone, preferred_element_type=jnp.float32)
            resid = right_side - solution - product
        collected.append(jnp.sum(resid * resid, axis=0))
        solution = solution + precondition(resid, precond)
    squares = jnp.pad(jnp.stack(collected), ((0, 16 - ITERS), (0, 0)))
    squares = gather(squares, rows_axis, cols_axis, 1).reshape(-1, 16, squares.shape[1])
    norms = jnp.sqrt(jnp.sum(squares[:, :ITERS], axis=0) / total)
    return (solution, norms)


def solution(mesh):
    in_specs = (P(("row", "col"), None), P(("row", "col"), None), P(("row", "col"), None, None))
    out_specs = (P(("row", "col"), None), P())
    body = functools.partial(local, mesh.shape["row"], mesh.shape["col"])
    return jax.shard_map(body, mesh=mesh, in_specs=in_specs, out_specs=out_specs, check_vma=False)
```
